32 devices in a mesh: gx: 4 (over x, core), gy: 8 (over z, y).
Axes of the slice: x: 2, y: 2, z: 4, core: 2. Of those that a mesh axis runs over, the one named last changes fastest.
Arguments:
- tokens: bfloat16 [256, 8192], P('gy', 'gx'), may hold values from -6 to 6
- up_old: bfloat16 [8192, 8192], P(('gx', 'gy')), may hold values from -0.0625 to 0.0625
- down_old: bfloat16 [8192, 8192], P(('gx', 'gy')), may hold values from -0.125 to 0.125
- old_slot: int32 [64], replicated, may hold values from 0 to 63, as said below
- new_owner: int32 [64], replicated, may hold values from 0 to 31, as said below
- hot_rank: int32 [64], replicated, may hold values from 0 to 1, as said below
- route: int32 [256], replicated, may hold values from 0 to 255, each once
Outputs:
- up_new: bfloat16 [8192, 8192], P(('gx', 'gy'))
- down_new: bfloat16 [8192, 8192], P(('gx', 'gy'))
- mixed: bfloat16 [256, 8192], P('gy', 'gx')
The draws below stay inside these ranges and needn't reach their ends.
Inputs may be any that keep to these rules, and one draw needn't show every extreme that they name: `old_slot`: each slot number appears exactly once. `new_owner`: each device index is the new owner of exactly 2 blocks. `hot_rank`: the blocks of one new owner have distinct ranks.
All inputs are finite; a program needn't handle non-finite values.
Results may differ from the reference program's by a relative error of at most 0.0049.
Values may be sent and summed in bfloat16 or wider, within the bound.
No kernel may reach another device: no remote copies, remote signals or barrier semaphores. Data moves between devices by JAX's collectives and lax.ppermute only.
A program may use at most 128 MiB of HBM per device.

```python
import jax
import jax.numpy as jnp
from jax import lax

D = 8192
BLOCK = 128
BLK_DEV = 2
FF = 8192
NBLK = 64
TOKENS = 256


def draw_old_slot(key, part):
    return jax.random.permutation(jax.random.fold_in(key, 11), NBLK).astype(jnp.int32)


def shared_order(key):
    return jax.random.permutation(jax.random.fold_in(key, 23), NBLK).astype(jnp.int32)


def draw_new_owner(key, part):
    return (shared_order(key) // BLK_DEV).astype(jnp.int32)


def draw_hot_rank(key, part):
    return (shared_order(key) % BLK_DEV).astype(jnp.int32)


def levels(stream_key, shape, cuts, least, high):
    factor_of, own = 1.0, jax.random.fold_in(stream_key, 6)
    for axis_at, blocks in cuts:
        draws = jnp.exp(jax.random.uniform(jax.random.fold_in(own, axis_at), (blocks,), jnp.float32, least / len(cuts), high / len(cuts)))
        factor_of = factor_of * jnp.repeat(draws, shape[axis_at] // blocks).reshape([-1 if axis == axis_at else 1 for axis in range(len(shape))])
    return factor_of


def scatter_about(rng, shape, width, most, cuts=(), held_as=jnp.bfloat16):
    factor_of = levels(rng, shape, cuts, -0.22, 0.18) if cuts else 1.0
    values = jax.random.normal(rng, shape, jnp.float32) * width * factor_of
    return jnp.minimum(jnp.maximum(values, -most), most).astype(held_as)


def setup_inputs(seed: int = 0) -> dict:
    key_list = jax.random.split(jax.random.key(seed), 8)
    return {
        "tokens": scatter_about(key_list[0], (TOKENS, D), 1.0, 6.0, ((0, 8), (1, 4))),
        "up_old": scatter_about(key_list[1], (FF, D), D ** -0.5, 0.0625, ((0, 32),)),
        "down_old": scatter_about(key_list[2], (FF, D), (FF // 4) ** -0.5, 0.125, ((0, 32),)),
        "old_slot": draw_old_slot(jax.random.fold_in(key_list[7], 71), 0),
        "new_owner": draw_new_owner(jax.random.fold_in(key_list[7], 71), 0),
        "hot_rank": draw_hot_rank(jax.random.fold_in(key_list[7], 71), 0),
        "route": jax.random.permutation(key_list[6], TOKENS).astype(jnp.int32),
    }


def reference(tokens, up_old, down_old, old_slot, new_owner, hot_rank, route):
    new_slot = (new_owner * BLK_DEV + hot_rank).astype(jnp.int32)
    source = jnp.zeros((NBLK,), jnp.int32).at[new_slot].set(old_slot.astype(jnp.int32))
    up_new = up_old.reshape(NBLK, BLOCK, D)[source].reshape(FF, D)
    down_new = down_old.reshape(NBLK, BLOCK, D)[source].reshape(FF, D)
    ordered = tokens[route.astype(jnp.int32)]
    pre = lax.dot_general(ordered, up_old, (((1,), (1,)), ((), ())), preferred_element_type=jnp.float32)
    hidden = jax.nn.gelu(pre, approximate=False).astype(jnp.bfloat16)
    mixed = jnp.dot(hidden, down_old, preferred_element_type=jnp.float32).astype(jnp.bfloat16)
    return up_new, down_new, mixed
```

```python
import functools

import jax
import jax.numpy as jnp
from jax import lax
from jax.experimental import pallas as pl
from jax.experimental.pallas import tpu as pltpu
from jax.sharding import PartitionSpec as P


BLOCK = 128
AXES = ("gx", "gy")
CHUNKS = 2
SPARE = 2
STEP = 2


ANY = pl.BlockSpec(memory_space=pl.ANY)
VMEM = pl.BlockSpec(memory_space=pltpu.VMEM)
SMEM = pl.BlockSpec(memory_space=pltpu.SMEM)


def run_all(copies):
    for copy in copies:
        copy.start()
    for copy in copies:
        copy.wait()


def cost(bytes_moved):
    return pl.CostEstimate(flops=bytes_moved * 8, bytes_accessed=bytes_moved, transcendentals=0)


def cut(rows, column, columns):
    held, group, r, _ = rows.shape

    def body(rows_ref, out_ref, sems):
        run_all([
            pltpu.make_async_copy(rows_ref.at[k, :, :, pl.ds(column, columns)], out_ref.at[:, k], sems.at[k])
            for k in range(held)
        ])

    return pl.pallas_call(
        body,
        out_shape=jax.ShapeDtypeStruct((group, held, r, columns), rows.dtype),
        in_specs=[ANY],
        out_specs=VMEM,
        scratch_shapes=[pltpu.SemaphoreType.DMA((held,))],
        cost_estimate=cost(4 * group * held * r * columns),
        name="cut",
    )(rows)


def pick(index, *pools):
    count, tail = index.shape[0], pools[0].shape[1:]

    def body(index_ref, *refs):
        pool_refs, out_ref, sems = refs[: len(pools)], refs[-2], refs[-1]

        def fetch(i, carry):
            at, first = index_ref[i], 0
            for ref in pool_refs:
                size = ref.shape[0]

                @pl.when((at >= first) & (at < first + size))
                def _(ref=ref, first=first):
                    pltpu.make_async_copy(ref.at[at - first], out_ref.at[i], sems.at[i]).start()

                first += size
            return carry

        def settle(i, carry):
            pltpu.make_async_copy(pool_refs[0].at[0], out_ref.at[i], sems.at[i]).wait()
            return carry

        lax.fori_loop(0, count, fetch, 0)
        lax.fori_loop(0, count, settle, 0)

    size = count * tail[0] * tail[1]
    return pl.pallas_call(
        body,
        out_shape=jax.ShapeDtypeStruct((count, *tail), pools[0].dtype),
        in_specs=[SMEM] + [ANY] * len(pools),
        out_specs=VMEM,
        scratch_shapes=[pltpu.SemaphoreType.DMA((count,))],
        cost_estimate=cost(4 * size),
        name="pick",
    )(index, *pools)


def put(landed, column, whole, shape):
    group, held, r, columns = landed.shape

    def body(landed_ref, *refs):
        out_ref, sems = refs[-2], refs[-1]
        run_all([
            pltpu.make_async_copy(landed_ref.at[:, k], out_ref.at[k, :, :, pl.ds(column, columns)], sems.at[k])
            for k in range(held)
        ])

    extra = [] if whole is None else [whole]
    return pl.pallas_call(
        body,
        out_shape=jax.ShapeDtypeStruct(shape, landed.dtype),
        in_specs=[VMEM] + [ANY] * len(extra),
        out_specs=ANY,
        scratch_shapes=[pltpu.SemaphoreType.DMA((held,))],
        input_output_aliases={1: 0} if extra else {},
        cost_estimate=cost(4 * group * held * r * columns),
        name="put",
    )(landed, *extra)


def plan(old_slot, new_owner, hot_rank, held, nx, ny):
    half = ny // 2
    size = nx * half * held

    def place(slot):
        device, k = lax.div(slot, held), lax.rem(slot, held)
        x, y = lax.div(device, ny), lax.rem(device, ny)
        return lax.div(y, half) * size + (x * half + lax.rem(y, half)) * held + k

    target, origin = place(new_owner * held + hot_rank), place(old_slot)
    at = jnp.arange(2 * size, dtype=jnp.int32)
    found = jnp.sum(jnp.where(target[None, :] == at[:, None], origin[None, :], 0), axis=1).reshape(2, size)
    side = jnp.arange(2, dtype=jnp.int32)[:, None]
    crosses = lax.div(found, size) != side
    within = lax.rem(found, size)
    i = jnp.arange(size, dtype=jnp.int32)
    rank = jnp.sum(jnp.where((i[None, :] < i[:, None])[None] & crosses[:, None, :], 1, 0), axis=2)
    land = jnp.where(crosses, size + rank, within)
    taken = (rank[:, None, :] == i[None, :, None]) & crosses[:, None, :]
    send = jnp.sum(jnp.where(taken, within[:, None, :], 0), axis=2)[::-1]
    return send.astype(jnp.int32), land.astype(jnp.int32), jnp.sum(crosses[0].astype(jnp.int32))


def relocate(arrays, old_slot, new_owner, hot_rank, nx, ny):
    half, width = ny // 2, arrays[0].shape[1]
    held = arrays[0].shape[0] // BLOCK
    group = nx * half
    r, size = BLOCK // group, group * held
    fixed = min(size, size // 2 + SPARE)
    columns = width // CHUNKS
    halves = [[x * ny + h * half + y for x in range(nx) for y in range(half)] for h in range(2)]
    across = [(d, d - d % ny + (d % ny + half) % ny) for d in range(nx * ny)]
    side = lax.div(lax.axis_index("gy"), half)

    sends, lands, crossing = plan(old_slot, new_owner, hot_rank, held, nx, ny)
    send = lax.dynamic_index_in_dim(sends, side, keepdims=False)
    land = lax.dynamic_index_in_dim(lands, side, keepdims=False)

    def swap(x):
        return lax.all_to_all(x, AXES, split_axis=0, concat_axis=0, tiled=True, axis_index_groups=halves)

    def spill(own, received):
        def step(i, extra):
            some = pick(lax.dynamic_slice_in_dim(padded, fixed + i * STEP, STEP), own)
            return lax.dynamic_update_slice_in_dim(extra, lax.ppermute(some, AXES, across), i * STEP, 0)

        steps = -(-(size - fixed) // STEP)
        padded = jnp.concatenate([send, jnp.zeros((STEP,), jnp.int32)])
        extra = jnp.zeros((steps * STEP, *own.shape[1:]), own.dtype)
        extra = lax.fori_loop(0, lax.div(crossing - fixed + STEP - 1, STEP), step, extra)
        return pick(land, own, received, extra)

    pieces = [(a, c * columns) for c in range(CHUNKS) for a in range(len(arrays))]
    split = [x.reshape(held, group, r, width) for x in arrays]
    out = [None] * len(arrays)
    count = len(pieces)
    own, received, landed = [None] * count, [None] * count, [None] * count

    def spread(c, *after):
        a, column = pieces[c]
        mine = lax.optimization_barrier((cut(split[a], column, columns), *after))[0]
        own[c] = swap(mine).reshape(size, r, columns)

    def cross(c):
        chosen = pick(send[:fixed], own[c])
        received[c] = lax.ppermute(chosen, AXES, across)
        return chosen

    def gather(c, *after):
        ordered = lax.cond(crossing <= fixed, functools.partial(pick, land), spill, own[c], received[c])
        ordered = lax.optimization_barrier((ordered, *after))[0]
        landed[c] = swap(ordered.reshape(group, held, r, columns))

    spread(0)
    first = cross(0)
    spread(1, own[0], first)
    for c in range(count):
        if c + 1 < count:
            chosen = cross(c + 1)
        if c + 2 < count:
            spread(c + 2, own[c + 1], chosen, *([landed[c - 1]] if c else []))
        gather(c, *([own[c + 2]] if c + 2 < count else []), *([landed[c - 1]] if c else []))
    for c, (a, column) in enumerate(pieces):
        out[a] = put(landed[c], column, out[a], split[a].shape)
    return tuple(x.reshape(held * BLOCK, width) for x in out)


def bits_of(n):
    return [1 << k for k in range(n.bit_length() - 1)]


def reversed_bits(i, n):
    bits = bits_of(n)
    return sum(lax.div(i, b) % 2 * (n // 2 // b) for b in bits) if bits else i


def pairs(axis, n, bit):
    return dict(axis_name=axis, perm=[(i, i ^ bit) for i in range(n)])


def project_up(x, rows, up):
    blocks, (count, feature) = len(rows), rows[0].shape
    hidden = up.shape[0]
    piece = min(feature, 512)

    def body(x_ref, *refs):
        row_refs, up_ref, out_ref = refs[:blocks], refs[blocks], refs[blocks + 1]
        out_ref[...] = jnp.zeros_like(out_ref)
        for j in range(blocks):
            first = (x_ref[0] ^ j) * feature

            def step(i, carry, j=j, first=first):
                at = pl.multiple_of(i * piece, piece)
                out_ref[...] += lax.dot_general(
                    row_refs[j][:, pl.ds(at, piece)],
                    up_ref[:, pl.ds(pl.multiple_of(first + at, piece), piece)],
                    (((1,), (1,)), ((), ())),
                    preferred_element_type=jnp.float32,
                )
                return carry

            lax.fori_loop(0, feature // piece, step, 0)

    return pl.pallas_call(
        body,
        out_shape=jax.ShapeDtypeStruct((count, hidden), jnp.float32),
        in_specs=[SMEM] + [VMEM] * (blocks + 1),
        out_specs=VMEM,
        cost_estimate=cost(4 * blocks * count * feature),
        name="project_up",
    )(x, *rows, up)


def project_down(x, hidden, down, blocks):
    count, feature = hidden.shape[0], down.shape[1] // blocks
    piece = min(feature, 512)

    def body(x_ref, hidden_ref, down_ref, keep_ref, send_ref):
        for j in range(blocks):
            first = (x_ref[0] ^ j) * feature

            def step(i, carry, j=j, first=first):
                at = pl.multiple_of(i * piece, piece)
                part = jnp.dot(
                    hidden_ref[...],
                    down_ref[:, pl.ds(pl.multiple_of(first + at, piece), piece)],
                    preferred_element_type=jnp.float32,
                )
                into = send_ref if j % 2 else keep_ref
                into[j // 2, :, pl.ds(at, piece)] = part
                return carry

            lax.fori_loop(0, feature // piece, step, 0)

    shape = (blocks // 2, count, feature)
    return pl.pallas_call(
        body,
        out_shape=(jax.ShapeDtypeStruct(shape, jnp.float32),) * 2,
        in_specs=[SMEM, VMEM, VMEM],
        out_specs=(VMEM, VMEM),
        cost_estimate=cost(8 * blocks * count * feature),
        name="project_down",
    )(x, hidden, down)


def layer(tokens, up, down, route, nx, ny):
    x, y = lax.axis_index("gx"), lax.axis_index("gy")
    held = tokens.shape[0]

    rows = tokens
    for bit in reversed(bits_of(ny)):
        rows = jnp.concatenate([rows, lax.ppermute(rows, **pairs("gy", ny, bit))])
    every = {0: rows}
    for bit in reversed(bits_of(nx)):
        every |= {j ^ bit: lax.ppermute(part, **pairs("gx", nx, bit)) for j, part in every.items()}

    at = jnp.arange(ny, dtype=jnp.int32)
    wanted = reversed_bits(at, ny) ^ y
    token = jnp.sum(jnp.where(wanted[:, None, None] == at[None, :, None], route.reshape(1, ny, held), 0), axis=1)
    index = (reversed_bits(lax.div(token, held) ^ y, ny) * held + lax.rem(token, held)).reshape(-1)

    own = x.reshape(1).astype(jnp.int32)
    pre = project_up(own, [every[j] for j in range(nx)], up)
    hidden = jax.nn.gelu(pre, approximate=False).astype(jnp.bfloat16)
    hidden = hidden.at[index].get(mode="promise_in_bounds")
    keep, send = project_down(own, hidden, down, nx)
    for bit in bits_of(nx):
        got = lax.ppermute(send, **pairs("gx", nx, bit))
        if 2 * bit < nx:
            send = (keep[1::2] + got[1::2]).astype(jnp.bfloat16)
            keep = keep[::2] + got[::2]
        else:
            total = keep[0] + got[0]
    for bit in bits_of(ny):
        here, there = jnp.split(total, 2)
        total = here + lax.ppermute(there, **pairs("gy", ny, bit))
    return total.astype(jnp.bfloat16)


def solution(mesh):
    nx, ny = mesh.shape["gx"], mesh.shape["gy"]

    def shards(tokens, up_old, down_old, old_slot, new_owner, hot_rank, route):
        mixed = layer(tokens, up_old, down_old, route, nx, ny)
        up_new, down_new = relocate((up_old, down_old), old_slot, new_owner, hot_rank, nx, ny)
        return (up_new, down_new, mixed)

    in_specs = (P("gy", "gx"), P(AXES, None), P(AXES, None), P(), P(), P(), P())
    out_specs = (P(AXES, None), P(AXES, None), P("gy", "gx"))
    return jax.shard_map(shards, mesh=mesh, in_specs=in_specs, out_specs=out_specs, check_vma=False)
```

```python
import functools

import jax
import jax.numpy as jnp
from jax import lax
from jax.experimental import pallas as pl
from jax.experimental.pallas import tpu as pltpu
from jax.sharding import PartitionSpec as P


BLOCK = 128
AXES = ("gx", "gy")
LANES = 128
SHORT = 3 / 8
SPARE = 2
STEP = 2


ANY = pl.BlockSpec(memory_space=pl.ANY)
VMEM = pl.BlockSpec(memory_space=pltpu.VMEM)
SMEM = pl.BlockSpec(memory_space=pltpu.SMEM)


def run_all(copies):
    for copy in copies:
        copy.start()
    for copy in copies:
        copy.wait()


def cost(bytes_moved):
    return pl.CostEstimate(flops=bytes_moved * 8, bytes_accessed=bytes_moved, transcendentals=0)


def cut(rows, column, columns):
    held, group, r, _ = rows.shape

    def body(rows_ref, out_ref, sems):
        run_all([
            pltpu.make_async_copy(rows_ref.at[k, :, :, pl.ds(column, columns)], out_ref.at[:, k], sems.at[k])
            for k in range(held)
        ])

    return pl.pallas_call(
        body,
        out_shape=jax.ShapeDtypeStruct((group, held, r, columns), rows.dtype),
        in_specs=[ANY],
        out_specs=VMEM,
        scratch_shapes=[pltpu.SemaphoreType.DMA((held,))],
        cost_estimate=cost(4 * group * held * r * columns),
        name="cut",
    )(rows)


def pick(index, *pools):
    count, tail = index.shape[0], pools[0].shape[1:]

    def body(index_ref, *refs):
        pool_refs, out_ref, sems = refs[: len(pools)], refs[-2], refs[-1]

        def fetch(i, carry):
            at, first = index_ref[i], 0
            for ref in pool_refs:
                size = ref.shape[0]

                @pl.when((at >= first) & (at < first + size))
                def _(ref=ref, first=first):
                    pltpu.make_async_copy(ref.at[at - first], out_ref.at[i], sems.at[i]).start()

                first += size
            return carry

        def settle(i, carry):
            pltpu.make_async_copy(pool_refs[0].at[0], out_ref.at[i], sems.at[i]).wait()
            return carry

        lax.fori_loop(0, count, fetch, 0)
        lax.fori_loop(0, count, settle, 0)

    size = count * tail[0] * tail[1]
    return pl.pallas_call(
        body,
        out_shape=jax.ShapeDtypeStruct((count, *tail), pools[0].dtype),
        in_specs=[SMEM] + [ANY] * len(pools),
        out_specs=VMEM,
        scratch_shapes=[pltpu.SemaphoreType.DMA((count,))],
        cost_estimate=cost(4 * size),
        name="pick",
    )(index, *pools)


def put(landed, column, whole, shape):
    group, held, r, columns = landed.shape

    def body(landed_ref, *refs):
        out_ref, sems = refs[-2], refs[-1]
        run_all([
            pltpu.make_async_copy(landed_ref.at[:, k], out_ref.at[k, :, :, pl.ds(column, columns)], sems.at[k])
            for k in range(held)
        ])

    extra = [] if whole is None else [whole]
    return pl.pallas_call(
        body,
        out_shape=jax.ShapeDtypeStruct(shape, landed.dtype),
        in_specs=[VMEM] + [ANY] * len(extra),
        out_specs=ANY,
        scratch_shapes=[pltpu.SemaphoreType.DMA((held,))],
        input_output_aliases={1: 0} if extra else {},
        cost_estimate=cost(4 * group * held * r * columns),
        name="put",
    )(landed, *extra)


def plan(old_slot, new_owner, hot_rank, held, nx, ny):
    half = ny // 2
    size = nx * half * held

    def place(slot):
        device, k = lax.div(slot, held), lax.rem(slot, held)
        x, y = lax.div(device, ny), lax.rem(device, ny)
        return lax.div(y, half) * size + (x * half + lax.rem(y, half)) * held + k

    target, origin = place(new_owner * held + hot_rank), place(old_slot)
    at = jnp.arange(2 * size, dtype=jnp.int32)
    found = jnp.sum(jnp.where(target[None, :] == at[:, None], origin[None, :], 0), axis=1).reshape(2, size)
    side = jnp.arange(2, dtype=jnp.int32)[:, None]
    crosses = lax.div(found, size) != side
    within = lax.rem(found, size)
    i = jnp.arange(size, dtype=jnp.int32)
    rank = jnp.sum(jnp.where((i[None, :] < i[:, None])[None] & crosses[:, None, :], 1, 0), axis=2)
    land = jnp.where(crosses, size + rank, within)
    taken = (rank[:, None, :] == i[None, :, None]) & crosses[:, None, :]
    send = jnp.sum(jnp.where(taken, within[:, None, :], 0), axis=2)[::-1]
    return send.astype(jnp.int32), land.astype(jnp.int32), jnp.sum(crosses[0].astype(jnp.int32))


def relocate(arrays, old_slot, new_owner, hot_rank, nx, ny):
    half, width = ny // 2, arrays[0].shape[1]
    held = arrays[0].shape[0] // BLOCK
    group = nx * half
    r, size = BLOCK // group, group * held
    fixed = min(size, size // 2 + SPARE)
    short = max(LANES, int(width * SHORT) // LANES * LANES)
    halves = [[x * ny + h * half + y for x in range(nx) for y in range(half)] for h in range(2)]
    across = [(d, d - d % ny + (d % ny + half) % ny) for d in range(nx * ny)]
    side = lax.div(lax.axis_index("gy"), half)

    sends, lands, crossing = plan(old_slot, new_owner, hot_rank, held, nx, ny)
    send = lax.dynamic_index_in_dim(sends, side, keepdims=False)
    land = lax.dynamic_index_in_dim(lands, side, keepdims=False)

    def swap(x):
        return lax.all_to_all(x, AXES, split_axis=0, concat_axis=0, tiled=True, axis_index_groups=halves)

    def spill(own, received):
        def step(i, extra):
            some = pick(lax.dynamic_slice_in_dim(padded, fixed + i * STEP, STEP), own)
            return lax.dynamic_update_slice_in_dim(extra, lax.ppermute(some, AXES, across), i * STEP, 0)

        steps = -(-(size - fixed) // STEP)
        padded = jnp.concatenate([send, jnp.zeros((STEP,), jnp.int32)])
        extra = jnp.zeros((steps * STEP, *own.shape[1:]), own.dtype)
        extra = lax.fori_loop(0, lax.div(crossing - fixed + STEP - 1, STEP), step, extra)
        return pick(land, own, received, extra)

    pieces = [(0, 0, short), (0, short, width - short), (1, 0, width - short), (1, width - short, short)]
    split = [x.reshape(held, group, r, width) for x in arrays]
    out = [None] * len(arrays)
    count = len(pieces)
    own, received, landed = [None] * count, [None] * count, [None] * count

    def spread(c, *after):
        a, column, columns = pieces[c]
        mine = lax.optimization_barrier((cut(split[a], column, columns), *after))[0]
        own[c] = swap(mine).reshape(size, r, columns)

    def cross(c):
        chosen = pick(send[:fixed], own[c])
        received[c] = lax.ppermute(chosen, AXES, across)
        return chosen

    def gather(c, *after):
        ordered = lax.cond(crossing <= fixed, functools.partial(pick, land), spill, own[c], received[c])
        ordered = lax.optimization_barrier((ordered, *after))[0]
        landed[c] = swap(ordered.reshape(group, held, r, -1))

    spread(0)
    for c in range(count):
        spread(c, *([own[c - 1]] if c else []))
        cross(c)
    for c in range(count):
        gather(c, *([landed[c - 1]] if c else []))
    for c, (a, column, _) in enumerate(pieces):
        out[a] = put(landed[c], column, out[a], split[a].shape)
    return tuple(x.reshape(held * BLOCK, width) for x in out)


def bits_of(n):
    return [1 << k for k in range(n.bit_length() - 1)]


def reversed_bits(i, n):
    bits = bits_of(n)
    return sum(lax.div(i, b) % 2 * (n // 2 // b) for b in bits) if bits else i


def pairs(axis, n, bit):
    return dict(axis_name=axis, perm=[(i, i ^ bit) for i in range(n)])


def project_up(x, rows, up):
    blocks, (count, feature) = len(rows), rows[0].shape
    hidden = up.shape[0]
    piece = min(feature, 512)

    def body(x_ref, *refs):
        row_refs, up_ref, out_ref = refs[:blocks], refs[blocks], refs[blocks + 1]
        out_ref[...] = jnp.zeros_like(out_ref)
        for j in range(blocks):
            first = (x_ref[0] ^ j) * feature

            def step(i, carry, j=j, first=first):
                at = pl.multiple_of(i * piece, piece)
                out_ref[...] += lax.dot_general(
                    row_refs[j][:, pl.ds(at, piece)],
                    up_ref[:, pl.ds(pl.multiple_of(first + at, piece), piece)],
                    (((1,), (1,)), ((), ())),
                    preferred_element_type=jnp.float32,
                )
                return carry

            lax.fori_loop(0, feature // piece, step, 0)

    return pl.pallas_call(
        body,
        out_shape=jax.ShapeDtypeStruct((count, hidden), jnp.float32),
        in_specs=[SMEM] + [VMEM] * (blocks + 1),
        out_specs=VMEM,
        cost_estimate=cost(4 * blocks * count * feature),
        name="project_up",
    )(x, *rows, up)


def project_down(x, hidden, down, blocks):
    count, feature = hidden.shape[0], down.shape[1] // blocks
    piece = min(feature, 512)

    def body(x_ref, hidden_ref, down_ref, keep_ref, send_ref):
        for j in range(blocks):
            first = (x_ref[0] ^ j) * feature

            def step(i, carry, j=j, first=first):
                at = pl.multiple_of(i * piece, piece)
                part = jnp.dot(
                    hidden_ref[...],
                    down_ref[:, pl.ds(pl.multiple_of(first + at, piece), piece)],
                    preferred_element_type=jnp.float32,
                )
                into = send_ref if j % 2 else keep_ref
                into[j // 2, :, pl.ds(at, piece)] = part
                return carry

            lax.fori_loop(0, feature // piece, step, 0)

    shape = (blocks // 2, count, feature)
    return pl.pallas_call(
        body,
        out_shape=(jax.ShapeDtypeStruct(shape, jnp.float32),) * 2,
        in_specs=[SMEM, VMEM, VMEM],
        out_specs=(VMEM, VMEM),
        cost_estimate=cost(8 * blocks * count * feature),
        name="project_down",
    )(x, hidden, down)


def layer(tokens, up, down, route, nx, ny):
    x, y = lax.axis_index("gx"), lax.axis_index("gy")
    held = tokens.shape[0]

    rows = tokens
    for bit in reversed(bits_of(ny)):
        rows = jnp.concatenate([rows, lax.ppermute(rows, **pairs("gy", ny, bit))])
    every = {0: rows}
    for bit in reversed(bits_of(nx)):
        every |= {j ^ bit: lax.ppermute(part, **pairs("gx", nx, bit)) for j, part in every.items()}

    at = jnp.arange(ny, dtype=jnp.int32)
    wanted = reversed_bits(at, ny) ^ y
    token = jnp.sum(jnp.where(wanted[:, None, None] == at[None, :, None], route.reshape(1, ny, held), 0), axis=1)
    index = (reversed_bits(lax.div(token, held) ^ y, ny) * held + lax.rem(token, held)).reshape(-1)

    own = x.reshape(1).astype(jnp.int32)
    pre = project_up(own, [every[j] for j in range(nx)], up)
    hidden = jax.nn.gelu(pre, approximate=False).astype(jnp.bfloat16)
    hidden = hidden.at[index].get(mode="promise_in_bounds")
    keep, send = project_down(own, hidden, down, nx)
    for bit in bits_of(nx):
        got = lax.ppermute(send, **pairs("gx", nx, bit))
        if 2 * bit < nx:
            send = (keep[1::2] + got[1::2]).astype(jnp.bfloat16)
            keep = keep[::2] + got[::2]
        else:
            total = keep[0] + got[0]
    for bit in bits_of(ny):
        here, there = jnp.split(total, 2)
        total = here + lax.ppermute(there, **pairs("gy", ny, bit))
    return total.astype(jnp.bfloat16)


def solution(mesh):
    nx, ny = mesh.shape["gx"], mesh.shape["gy"]

    def shards(tokens, up_old, down_old, old_slot, new_owner, hot_rank, route):
        mixed = layer(tokens, up_old, down_old, route, nx, ny)
        up_new, down_new = relocate((up_old, down_old), old_slot, new_owner, hot_rank, nx, ny)
        return (up_new, down_new, mixed)

    in_specs = (P("gy", "gx"), P(AXES, None), P(AXES, None), P(), P(), P(), P())
    out_specs = (P(AXES, None), P(AXES, None), P("gy", "gx"))
    return jax.shard_map(shards, mesh=mesh, in_specs=in_specs, out_specs=out_specs, check_vma=False)
```

```python
import functools

import jax
import jax.numpy as jnp
from jax import lax
from jax.experimental import pallas as pl
from jax.experimental.pallas import tpu as pltpu
from jax.sharding import PartitionSpec as P


BLOCK = 128
AXES = ("gx", "gy")
LANES = 128
FIRST = 7 / 16
LAST = 3 / 8
SPARE = 2
STEP = 2


ANY = pl.BlockSpec(memory_space=pl.ANY)
VMEM = pl.BlockSpec(memory_space=pltpu.VMEM)
SMEM = pl.BlockSpec(memory_space=pltpu.SMEM)


def run_all(copies):
    for copy in copies:
        copy.start()
    for copy in copies:
        copy.wait()


def cost(bytes_moved):
    return pl.CostEstimate(flops=bytes_moved * 8, bytes_accessed=bytes_moved, transcendentals=0)


def cut(rows, column, columns):
    held, group, r, _ = rows.shape

    def body(rows_ref, out_ref, sems):
        run_all([
            pltpu.make_async_copy(rows_ref.at[k, :, :, pl.ds(column, columns)], out_ref.at[:, k], sems.at[k])
            for k in range(held)
        ])

    return pl.pallas_call(
        body,
        out_shape=jax.ShapeDtypeStruct((group, held, r, columns), rows.dtype),
        in_specs=[ANY],
        out_specs=VMEM,
        scratch_shapes=[pltpu.SemaphoreType.DMA((held,))],
        cost_estimate=cost(4 * group * held * r * columns),
        name="cut",
    )(rows)


def pick(index, *pools):
    count, tail = index.shape[0], pools[0].shape[1:]

    def body(index_ref, *refs):
        pool_refs, out_ref, sems = refs[: len(pools)], refs[-2], refs[-1]

        def fetch(i, carry):
            at, first = index_ref[i], 0
            for ref in pool_refs:
                size = ref.shape[0]

                @pl.when((at >= first) & (at < first + size))
                def _(ref=ref, first=first):
                    pltpu.make_async_copy(ref.at[at - first], out_ref.at[i], sems.at[i]).start()

                first += size
            return carry

        def settle(i, carry):
            pltpu.make_async_copy(pool_refs[0].at[0], out_ref.at[i], sems.at[i]).wait()
            return carry

        lax.fori_loop(0, count, fetch, 0)
        lax.fori_loop(0, count, settle, 0)

    size = count * tail[0] * tail[1]
    return pl.pallas_call(
        body,
        out_shape=jax.ShapeDtypeStruct((count, *tail), pools[0].dtype),
        in_specs=[SMEM] + [ANY] * len(pools),
        out_specs=VMEM,
        scratch_shapes=[pltpu.SemaphoreType.DMA((count,))],
        cost_estimate=cost(4 * size),
        name="pick",
    )(index, *pools)


def put(landed, column, whole, shape):
    group, held, r, columns = landed.shape

    def body(landed_ref, *refs):
        out_ref, sems = refs[-2], refs[-1]
        run_all([
            pltpu.make_async_copy(landed_ref.at[:, k], out_ref.at[k, :, :, pl.ds(column, columns)], sems.at[k])
            for k in range(held)
        ])

    extra = [] if whole is None else [whole]
    return pl.pallas_call(
        body,
        out_shape=jax.ShapeDtypeStruct(shape, landed.dtype),
        in_specs=[VMEM] + [ANY] * len(extra),
        out_specs=ANY,
        scratch_shapes=[pltpu.SemaphoreType.DMA((held,))],
        input_output_aliases={1: 0} if extra else {},
        cost_estimate=cost(4 * group * held * r * columns),
        name="put",
    )(landed, *extra)


def plan(old_slot, new_owner, hot_rank, held, nx, ny):
    half = ny // 2
    size = nx * half * held

    def place(slot):
        device, k = lax.div(slot, held), lax.rem(slot, held)
        x, y = lax.div(device, ny), lax.rem(device, ny)
        return lax.div(y, half) * size + (x * half + lax.rem(y, half)) * held + k

    target, origin = place(new_owner * held + hot_rank), place(old_slot)
    at = jnp.arange(2 * size, dtype=jnp.int32)
    found = jnp.sum(jnp.where(target[None, :] == at[:, None], origin[None, :], 0), axis=1).reshape(2, size)
    side = jnp.arange(2, dtype=jnp.int32)[:, None]
    crosses = lax.div(found, size) != side
    within = lax.rem(found, size)
    i = jnp.arange(size, dtype=jnp.int32)
    rank = jnp.sum(jnp.where((i[None, :] < i[:, None])[None] & crosses[:, None, :], 1, 0), axis=2)
    land = jnp.where(crosses, size + rank, within)
    taken = (rank[:, None, :] == i[None, :, None]) & crosses[:, None, :]
    send = jnp.sum(jnp.where(taken, within[:, None, :], 0), axis=2)[::-1]
    return send.astype(jnp.int32), land.astype(jnp.int32), jnp.sum(crosses[0].astype(jnp.int32))


def relocate(arrays, old_slot, new_owner, hot_rank, nx, ny):
    half, width = ny // 2, arrays[0].shape[1]
    held = arrays[0].shape[0] // BLOCK
    group = nx * half
    r, size = BLOCK // group, group * held
    fixed = min(size, size // 2 + SPARE)
    halves = [[x * ny + h * half + y for x in range(nx) for y in range(half)] for h in range(2)]
    across = [(d, d - d % ny + (d % ny + half) % ny) for d in range(nx * ny)]
    side = lax.div(lax.axis_index("gy"), half)

    sends, lands, crossing = plan(old_slot, new_owner, hot_rank, held, nx, ny)
    send = lax.dynamic_index_in_dim(sends, side, keepdims=False)
    land = lax.dynamic_index_in_dim(lands, side, keepdims=False)

    def swap(x):
        return lax.all_to_all(x, AXES, split_axis=0, concat_axis=0, tiled=True, axis_index_groups=halves)

    def spill(own, received):
        def step(i, extra):
            some = pick(lax.dynamic_slice_in_dim(padded, fixed + i * STEP, STEP), own)
            return lax.dynamic_update_slice_in_dim(extra, lax.ppermute(some, AXES, across), i * STEP, 0)

        steps = -(-(size - fixed) // STEP)
        padded = jnp.concatenate([send, jnp.zeros((STEP,), jnp.int32)])
        extra = jnp.zeros((steps * STEP, *own.shape[1:]), own.dtype)
        extra = lax.fori_loop(0, lax.div(crossing - fixed + STEP - 1, STEP), step, extra)
        return pick(land, own, received, extra)

    first, last = (max(LANES, int(width * part) // LANES * LANES) for part in (FIRST, LAST))
    pieces = [(0, 0, first), (0, first, width - first), (1, 0, width - last), (1, width - last, last)]
    split = [x.reshape(held, group, r, width) for x in arrays]
    out = [None] * len(arrays)
    count = len(pieces)
    own, received, landed = [None] * count, [None] * count, [None] * count

    def spread(c, *after):
        a, column, columns = pieces[c]
        mine = lax.optimization_barrier((cut(split[a], column, columns), *after))[0]
        own[c] = swap(mine).reshape(size, r, columns)

    def cross(c):
        chosen = pick(send[:fixed], own[c])
        received[c] = lax.ppermute(chosen, AXES, across)
        return chosen

    def gather(c, *after):
        ordered = lax.cond(crossing <= fixed, functools.partial(pick, land), spill, own[c], received[c])
        ordered = lax.optimization_barrier((ordered, *after))[0]
        landed[c] = swap(ordered.reshape(group, held, r, -1))

    spread(0)
    for c in range(count):
        spread(c, *([own[c - 1]] if c else []))
        cross(c)
    for c in range(count):
        gather(c, *([landed[c - 1]] if c else []))
    for c, (a, column, _) in enumerate(pieces):
        out[a] = put(landed[c], column, out[a], split[a].shape)
    return tuple(x.reshape(held * BLOCK, width) for x in out)


def bits_of(n):
    return [1 << k for k in range(n.bit_length() - 1)]


def reversed_bits(i, n):
    bits = bits_of(n)
    return sum(lax.div(i, b) % 2 * (n // 2 // b) for b in bits) if bits else i


def pairs(axis, n, bit):
    return dict(axis_name=axis, perm=[(i, i ^ bit) for i in range(n)])


def project_up(x, rows, up):
    blocks, (count, feature) = len(rows), rows[0].shape
    hidden = up.shape[0]
    piece = min(feature, 512)

    def body(x_ref, *refs):
        row_refs, up_ref, out_ref = refs[:blocks], refs[blocks], refs[blocks + 1]
        out_ref[...] = jnp.zeros_like(out_ref)
        for j in range(blocks):
            first = (x_ref[0] ^ j) * feature

            def step(i, carry, j=j, first=first):
                at = pl.multiple_of(i * piece, piece)
                out_ref[...] += lax.dot_general(
                    row_refs[j][:, pl.ds(at, piece)],
                    up_ref[:, pl.ds(pl.multiple_of(first + at, piece), piece)],
                    (((1,), (1,)), ((), ())),
                    preferred_element_type=jnp.float32,
                )
                return carry

            lax.fori_loop(0, feature // piece, step, 0)

    return pl.pallas_call(
        body,
        out_shape=jax.ShapeDtypeStruct((count, hidden), jnp.float32),
        in_specs=[SMEM] + [VMEM] * (blocks + 1),
        out_specs=VMEM,
        cost_estimate=cost(4 * blocks * count * feature),
        name="project_up",
    )(x, *rows, up)


def project_down(x, hidden, down, blocks):
    count, feature = hidden.shape[0], down.shape[1] // blocks
    piece = min(feature, 512)

    def body(x_ref, hidden_ref, down_ref, keep_ref, send_ref):
        for j in range(blocks):
            first = (x_ref[0] ^ j) * feature

            def step(i, carry, j=j, first=first):
                at = pl.multiple_of(i * piece, piece)
                part = jnp.dot(
                    hidden_ref[...],
                    down_ref[:, pl.ds(pl.multiple_of(first + at, piece), piece)],
                    preferred_element_type=jnp.float32,
                )
                into = send_ref if j % 2 else keep_ref
                into[j // 2, :, pl.ds(at, piece)] = part
                return carry

            lax.fori_loop(0, feature // piece, step, 0)

    shape = (blocks // 2, count, feature)
    return pl.pallas_call(
        body,
        out_shape=(jax.ShapeDtypeStruct(shape, jnp.float32),) * 2,
        in_specs=[SMEM, VMEM, VMEM],
        out_specs=(VMEM, VMEM),
        cost_estimate=cost(8 * blocks * count * feature),
        name="project_down",
    )(x, hidden, down)


def layer(tokens, up, down, route, nx, ny):
    x, y = lax.axis_index("gx"), lax.axis_index("gy")
    held = tokens.shape[0]

    rows = tokens
    for bit in reversed(bits_of(ny)):
        rows = jnp.concatenate([rows, lax.ppermute(rows, **pairs("gy", ny, bit))])
    every = {0: rows}
    for bit in reversed(bits_of(nx)):
        every |= {j ^ bit: lax.ppermute(part, **pairs("gx", nx, bit)) for j, part in every.items()}

    at = jnp.arange(ny, dtype=jnp.int32)
    wanted = reversed_bits(at, ny) ^ y
    token = jnp.sum(jnp.where(wanted[:, None, None] == at[None, :, None], route.reshape(1, ny, held), 0), axis=1)
    index = (reversed_bits(lax.div(token, held) ^ y, ny) * held + lax.rem(token, held)).reshape(-1)

    own = x.reshape(1).astype(jnp.int32)
    pre = project_up(own, [every[j] for j in range(nx)], up)
    hidden = jax.nn.gelu(pre, approximate=False).astype(jnp.bfloat16)
    hidden = hidden.at[index].get(mode="promise_in_bounds")
    keep, send = project_down(own, hidden, down, nx)
    for bit in bits_of(nx):
        got = lax.ppermute(send, **pairs("gx", nx, bit))
        if 2 * bit < nx:
            send = (keep[1::2] + got[1::2]).astype(jnp.bfloat16)
            keep = keep[::2] + got[::2]
        else:
            total = keep[0] + got[0]
    for bit in bits_of(ny):
        here, there = jnp.split(total, 2)
        if bit >= ny // 4:
            there = there.astype(jnp.bfloat16)
        total = here + lax.ppermute(there, **pairs("gy", ny, bit))
    return total.astype(jnp.bfloat16)


def solution(mesh):
    nx, ny = mesh.shape["gx"], mesh.shape["gy"]

    def shards(tokens, up_old, down_old, old_slot, new_owner, hot_rank, route):
        mixed = layer(tokens, up_old, down_old, route, nx, ny)
        up_new, down_new = relocate((up_old, down_old), old_slot, new_owner, hot_rank, nx, ny)
        return (up_new, down_new, mixed)

    in_specs = (P("gy", "gx"), P(AXES, None), P(AXES, None), P(), P(), P(), P())
    out_specs = (P(AXES, None), P(AXES, None), P("gy", "gx"))
    return jax.shard_map(shards, mesh=mesh, in_specs=in_specs, out_specs=out_specs, check_vma=False)
```
